32 devices in a mesh: row: 8 (over z, y), col: 4 (over x, core).
Axes of the slice: x: 2, y: 2, z: 4, core: 2. Of those that a mesh axis runs over, the one named last changes fastest.
Arguments:
- child_parent: int32 [4096], P(('row', 'col')), may hold values from 0 to 1023, as said below
- prefix_len: int32 [4096], P(('row', 'col')), may hold values from 1 to 40
- child_delta: bfloat16 [4096, 3584], P(('row', 'col')), may hold values from -6 to 6
- parent_hidden: bfloat16 [1024, 3584], P(('row', 'col')), may hold values from -6 to 6
- parent_cache: bfloat16 [1024, 2, 2, 128, 128], P(('row', 'col')), may hold values from -720 to 720
- prefix_cache: bfloat16 [32, 2, 2, 5120, 128], P(('row', 'col')), may hold values from -720 to 720
- norm_gain: float32 [3584], replicated, may hold values from 0.1 to 1.9
- w_query: bfloat16 [3584, 1792], replicated, may hold values from -0.09375 to 0.09375
- w_kv: bfloat16 [3584, 512], replicated, may hold values from -0.09375 to 0.09375
Outputs:
- context: bfloat16 [4096, 1792], P(('row', 'col'))
- child_kv: bfloat16 [4096, 512], P(('row', 'col'))
The draws below stay inside these ranges and needn't reach their ends.
Inputs may be any that keep to these rules, and one draw needn't show every extreme that they name: `child_parent`: each device's 128 children name exactly 32 parents held in each column of devices; the children of any one row of devices name exactly 16 parents held by any one device; one device's children name at most 4 parents held by one device, and exactly 4 for some pairs. Parent p is held by device p // 32, device index = row index * 4 + column index.
All inputs are finite; a program needn't handle non-finite values.
Results may differ from the reference program's by a relative error of at most 0.0085.
The reference program's roundings to bfloat16 on the way count: a program that leaves them out, or rounds other values in their place, can miss the bound.
Values may be sent and summed in bfloat16 or wider, within the bound.
No kernel may reach another device: no remote copies, remote signals or barrier semaphores. Data moves between devices by JAX's collectives and lax.ppermute only.
A program may use at most 256 MiB of HBM per device.

```python
import math
import jax
import jax.numpy as jnp
from jax import lax

D = 3584
QH = 14
KVH = 2
DH = 128
BLOCK = 128
PB = 40
C_DEV = 128
CHILDREN = 4096
PARENTS = 1024
N_ROW = 8
N_COL = 4


def draw_child_parent(key, part):
    device_count = N_ROW * N_COL
    half_span = C_DEV // (2 * N_COL)
    shift_reach = half_span % N_ROW if half_span % N_ROW else N_ROW
    key_shift, key_rows, key_cols, key_slots, key_local = jax.random.split(jax.random.fold_in(key, 11), 5)
    offsets = jnp.arange(half_span, dtype=jnp.int32)
    start_rows = jnp.arange(N_COL, dtype=jnp.int32)[:, None] * half_span
    base_rows = (start_rows + offsets[None, :]) % N_ROW
    shift_draw = jax.random.randint(key_shift, (N_ROW, N_COL, 1, 1), 0, shift_reach)
    first_cover = jnp.broadcast_to(base_rows, (N_ROW, N_COL, N_COL, half_span))
    second_cover = (first_cover + shift_draw) % N_ROW
    source_rows = jnp.concatenate([first_cover, second_cover], axis=3)
    row_order = jax.vmap(lambda one_key: jax.random.permutation(one_key, N_ROW))(jax.random.split(key_rows, N_ROW * N_COL))
    row_order = jnp.broadcast_to(row_order.reshape(N_ROW, N_COL, 1, N_ROW), (N_ROW, N_COL, N_COL, N_ROW))
    source_rows = jnp.take_along_axis(row_order, source_rows, axis=3)
    col_order = jax.vmap(lambda one_key: jax.random.permutation(one_key, N_COL))(jax.random.split(key_cols, N_ROW * N_COL))
    col_inverse = jnp.argsort(col_order.reshape(N_ROW, N_COL, N_COL), axis=-1).astype(jnp.int32)
    col_inverse = jnp.broadcast_to(col_inverse[..., None], (N_ROW, N_COL, N_COL, 2 * half_span))
    source_rows = jnp.take_along_axis(source_rows, col_inverse, axis=2)
    source_dev = source_rows * N_COL + jnp.arange(N_COL, dtype=jnp.int32)[None, :, None, None]
    source_dev = jnp.transpose(source_dev, (0, 2, 1, 3)).reshape(device_count, C_DEV)
    slot_order = jax.vmap(lambda one_key: jax.random.permutation(one_key, C_DEV))(jax.random.split(key_slots, device_count))
    source_dev = jnp.take_along_axis(source_dev, slot_order, axis=1)
    local_ids = jax.random.randint(key_local, (device_count, C_DEV), 0, C_DEV // 4)
    return (source_dev * (C_DEV // 4) + local_ids).reshape(device_count * C_DEV).astype(jnp.int32)


def spiked_draw(key, shape):
    key_base = jax.random.fold_in(key, 0)
    normal_part = jnp.clip(jax.random.normal(key_base, shape, jnp.float32), -6.0, 6.0)
    return normal_part.astype(jnp.bfloat16)


def draw_parent_cache(key, part):
    return spiked_draw(jax.random.fold_in(key, 31), (C_DEV // 4 * N_ROW * N_COL, 2, KVH, BLOCK, DH))


def draw_prefix_cache(key, part):
    return spiked_draw(jax.random.fold_in(key, 21), (N_ROW * N_COL, 2, KVH, PB * BLOCK, DH))


def set_ends(array, stream_key, least, largest):
    extent = array.shape
    spot = [jax.random.randint(jax.random.fold_in(stream_key, axis), (), 0, extent[axis]) for axis in range(len(extent))]
    array = array.at[tuple(spot)].set(least)
    longest = extent.index(max(extent))
    spot[longest] = (spot[longest] + 1) % extent[longest]
    return array.at[tuple(spot)].set(largest)


def block_levels(own_key, extent, cuts, smallest, largest):
    factor_of, own = 1.0, jax.random.fold_in(own_key, 6)
    for position, parts in cuts:
        draws = jnp.exp(jax.random.uniform(jax.random.fold_in(own, position), (parts,), jnp.float32, smallest / len(cuts), largest / len(cuts)))
        factor_of = factor_of * jnp.repeat(draws, extent[position] // parts).reshape([-1 if axis == position else 1 for axis in range(len(extent))])
    return factor_of


def gaussian(own_key, extent, deviation, limit, pieces=(), kind=jnp.bfloat16):
    array = deviation * jax.random.normal(own_key, extent, jnp.float32)
    if pieces:
        array = array * block_levels(own_key, extent, pieces, -0.22, 0.18)
    return jnp.clip(array, -limit, limit).astype(kind)


def setup_inputs(seed: int = 0) -> dict:
    splits = jax.random.split(jax.random.key(seed), 10)
    return {
        "child_parent": draw_child_parent(jax.random.fold_in(splits[9], 71), 0),
        "prefix_len": set_ends(jax.random.randint(splits[1], (CHILDREN,), 1, PB + 1), jax.random.fold_in(splits[1], 1), 1, PB).astype(jnp.int32),
        "child_delta": gaussian(splits[2], (CHILDREN, D), 1.0, 6.0, ((0, 32),)),
        "parent_hidden": gaussian(splits[3], (PARENTS, D), 1.0, 6.0, ((0, 32),)),
        "parent_cache": draw_parent_cache(jax.random.fold_in(splits[9], 71), 0),
        "prefix_cache": draw_prefix_cache(jax.random.fold_in(splits[9], 71), 0),
        "norm_gain": jnp.clip(1.0 + 0.18 * jax.random.normal(splits[6], (D,), jnp.float32), 0.1, 1.9),
        "w_query": gaussian(splits[7], (D, QH * DH), D ** -0.5, 0.09375),
        "w_kv": gaussian(splits[8], (D, 2 * KVH * DH), D ** -0.5, 0.09375),
    }


EPSILON = 1e-06

def decode_child(parent_rows, parent_blocks, delta_rows, block_counts, prefix_rows, norm_gain, w_query, w_kv):
    highest = lax.Precision.HIGHEST
    widened = parent_rows.astype(jnp.float32) + delta_rows.astype(jnp.float32)
    inverse = lax.rsqrt(lax.optimization_barrier(jnp.mean(widened * widened, axis=-1, keepdims=True)) + EPSILON)
    normed = (widened * inverse * norm_gain).astype(jnp.bfloat16)
    queries = jnp.dot(normed, w_query, preferred_element_type=jnp.float32).astype(jnp.bfloat16)
    new_kv = jnp.dot(normed, w_kv, preferred_element_type=jnp.float32).astype(jnp.bfloat16)
    child_count = parent_rows.shape[0]
    kv_heads = prefix_rows.shape[1]
    head_dim = prefix_rows.shape[-1]
    block_tokens = parent_blocks.shape[3]
    grouped = queries.astype(jnp.float32).reshape(child_count, kv_heads, -1, head_dim)
    scale_factor = 1.0 / math.sqrt(head_dim)
    prefix_keys = prefix_rows[0].astype(jnp.float32)
    score_pre = jnp.einsum('chgd,hld->hcgl', grouped, prefix_keys, precision=highest) * scale_factor
    key_positions = jnp.arange(prefix_keys.shape[1], dtype=jnp.int32)
    limits = block_counts * block_tokens
    in_prefix = key_positions[None, None, None, :] < limits[None, :, None, None]
    score_pre = jnp.where(in_prefix, score_pre, -jnp.inf)
    score_par = jnp.einsum('chgd,chtd->hcgt', grouped, parent_blocks[:, 0].astype(jnp.float32), precision=highest) * scale_factor
    top_score = jnp.maximum(lax.optimization_barrier(jnp.max(score_pre, axis=-1, keepdims=True)), lax.optimization_barrier(jnp.max(score_par, axis=-1, keepdims=True)))
    exp_pre = jnp.exp(score_pre - top_score)
    exp_par = jnp.exp(score_par - top_score)
    denominator = lax.optimization_barrier(jnp.sum(exp_pre, axis=-1, keepdims=True)) + lax.optimization_barrier(jnp.sum(exp_par, axis=-1, keepdims=True))
    weight_pre = (exp_pre / denominator).astype(jnp.bfloat16)
    weight_par = (exp_par / denominator).astype(jnp.bfloat16)
    context = jnp.einsum('hcgl,hld->chgd', weight_pre.astype(jnp.float32), prefix_rows[1].astype(jnp.float32), precision=highest)
    context = context + jnp.einsum('hcgt,chtd->chgd', weight_par.astype(jnp.float32), parent_blocks[:, 1].astype(jnp.float32), precision=highest)
    return (context.reshape(child_count, -1).astype(jnp.bfloat16), new_kv)

def reference(child_parent, prefix_len, child_delta, parent_hidden, parent_cache, prefix_cache, norm_gain, w_query, w_kv):

    def per_device(device):
        first_child = device * C_DEV
        parent_ids = lax.dynamic_slice_in_dim(child_parent, first_child, C_DEV, 0)
        block_counts = lax.dynamic_slice_in_dim(prefix_len, first_child, C_DEV, 0)
        delta_rows = lax.dynamic_slice_in_dim(child_delta, first_child, C_DEV, 0)
        prefix_rows = lax.dynamic_index_in_dim(prefix_cache, device, 0, keepdims=False)
        return decode_child(parent_hidden[parent_ids], parent_cache[parent_ids], delta_rows, block_counts, prefix_rows, norm_gain, w_query, w_kv)
    context, new_kv = lax.map(per_device, jnp.arange(N_ROW * N_COL, dtype=jnp.int32))
    return (context.reshape(CHILDREN, -1), new_kv.reshape(CHILDREN, -1))
```

```python
import functools
import math

import jax
import jax.numpy as jnp
from jax import lax
from jax.experimental import pallas as pl
from jax.experimental.pallas import tpu as pltpu
from jax.sharding import PartitionSpec as P

EPSILON = 1e-06
LOG2E = 1.4426950408889634
LOW = -1e30
CHILD_TILE = 32
CHUNK = 512
SLOT_UNROLL = 8

f32 = jnp.float32
bf16 = jnp.bfloat16
i32 = jnp.int32
VMEM = pl.BlockSpec(memory_space=pltpu.VMEM)
SMEM = pl.BlockSpec(memory_space=pltpu.SMEM)


def dot(a, b):
    return jnp.dot(a, b, preferred_element_type=f32)


def dot_nt(a, b):
    return lax.dot_general(a, b, (((1,), (1,)), ((), ())), preferred_element_type=f32)


def iota(shape, axis):
    return lax.broadcasted_iota(i32, shape, axis)


def onehot(mask):
    return jnp.where(mask, 1.0, 0.0).astype(bf16)


def to_column(row):
    n = row.shape[1]
    same = iota((n, n), 0) == iota((n, n), 1)
    return jnp.sum(jnp.where(same, jnp.broadcast_to(row, (n, n)), 0.0), axis=1, keepdims=True)


def box_rows(rows, parts, capacity):
    r = iota((rows, 1), 0)
    shift = (parts * capacity).bit_length() - 1
    device = lax.shift_right_logical(r, shift)
    within = lax.bitwise_and(r, parts * capacity - 1)
    part = lax.shift_right_logical(within, capacity.bit_length() - 1)
    rank = lax.bitwise_and(within, capacity - 1)
    return device * capacity + rank, part


def pack_matrix(rows, parts, capacity, slot_row):
    slot, part = box_rows(rows, parts, capacity)
    return jnp.concatenate(
        [onehot((slot_row == slot) & (part == p)) for p in range(parts)], axis=1
    )


def stack_parts(x, parts):
    width = x.shape[1] // parts
    return jnp.concatenate([x[:, p * width : (p + 1) * width] for p in range(parts)], axis=0)


def pack_kernel(parents, capacity, parts, slots, cp_ref, len_ref, delta_ref, box_ref, idx_ref, ids_ref):
    n = cp_ref.shape[1]
    ri, ci = iota((n, n), 0), iota((n, n), 1)
    cp = cp_ref[...].astype(f32)
    src = jnp.floor((cp + 0.5) * (1.0 / parents))
    loc = cp - src * parents
    src_col = to_column(src)
    rank = jnp.sum(jnp.where((src_col == src) & (ri < ci), 1.0, 0.0), axis=0, keepdims=True)
    slot = src * capacity + rank
    rows = box_ref.shape[0]
    pack = pack_matrix(rows, parts, capacity, slot.astype(i32))
    box_ref[...] = dot(pack, stack_parts(delta_ref[...], parts)).astype(bf16)

    slot_col = to_column(slot)
    loc_col = to_column(loc)
    ids_ref[...] = jnp.sum(
        jnp.where(slot_col == iota((n, slots), 1).astype(f32), loc_col, 0.0), axis=0, keepdims=True
    ).astype(i32)
    length = len_ref[...].astype(f32)
    len_col = to_column(length)
    srank = jnp.sum(
        jnp.where((len_col > length) | ((len_col == length) & (ri < ci)), 1.0, 0.0),
        axis=0,
        keepdims=True,
    )
    chosen = to_column(srank) == ci.astype(f32)
    sorted_slot = jnp.sum(jnp.where(chosen, slot_col, 0.0), axis=0, keepdims=True)
    sorted_len = jnp.sum(jnp.where(chosen, len_col, 0.0), axis=0, keepdims=True)
    device = jnp.floor((sorted_slot + 0.5) * (1.0 / capacity))
    base = device * (2 * capacity) + (sorted_slot - device * capacity)
    idx_ref[...] = jnp.concatenate(
        [base, sorted_len, srank, jnp.zeros((5, n), f32)], axis=0
    ).astype(i32)


def project_kernel(
    capacity, parts, box_ref, ids_ref, hidden_ref, gain_ref, wq_ref, wkv_ref, q_ref, qbox_ref, kv_ref, h_ref, n_ref
):
    slots = q_ref.shape[0]
    parents = hidden_ref.shape[0]
    rows, width = box_ref.shape
    features = hidden_ref.shape[1]
    ids_col = to_column(ids_ref[...].astype(f32)).astype(i32)
    pick = onehot(ids_col == iota((slots, parents), 1))
    s = iota((slots, 1), 0)
    base = (
        lax.shift_right_logical(s, capacity.bit_length() - 1) * (parts * capacity)
        + lax.bitwise_and(s, capacity - 1)
    )
    squares = jnp.zeros((slots, 1), f32)
    for p in range(parts):
        take = onehot(iota((slots, rows), 1) == base + p * capacity)
        cols = slice(p * width, (p + 1) * width)
        h = dot(pick, hidden_ref[:, cols]) + dot(take, box_ref[...])
        h_ref[:, cols] = h
        squares = squares + jnp.sum(h * h, axis=1, keepdims=True)
    inverse = lax.rsqrt(squares * (1.0 / features) + EPSILON)
    n_ref[...] = (h_ref[...] * inverse * gain_ref[...]).astype(bf16)
    step = 256
    for j in range(0, q_ref.shape[1], step):
        q_ref[:, j : j + step] = dot(n_ref[...], wq_ref[:, j : j + step]).astype(bf16)
    for j in range(0, kv_ref.shape[1], step):
        kv_ref[:, j : j + step] = dot(n_ref[...], wkv_ref[:, j : j + step]).astype(bf16)
    slot_row = iota((1, slots), 1)
    pack = pack_matrix(qbox_ref.shape[0], 2, capacity, slot_row)
    qbox_ref[...] = dot(pack, stack_parts(q_ref[...], 2)).astype(bf16)


def parent_kernel(capacity, scale, ids_ref, q_ref, kv_ref, cache_ref, out_ref, qs_ref, os_ref, ls_ref):
    slots, width = q_ref.shape
    head_dim = cache_ref.shape[-1]
    kv_heads = cache_ref.shape[2]
    group = width // (kv_heads * head_dim)
    for g in range(kv_heads):
        for h in range(group):
            c0 = (g * group + h) * head_dim
            qs_ref[g, pl.ds(h, slots, stride=8), :] = q_ref[:, c0 : c0 + head_dim].astype(f32)
        qs_ref[g, pl.ds(group, slots, stride=8), :] = jnp.zeros((slots, head_dim), f32)

    def step(i, carry):
        for u in range(SLOT_UNROLL):
            s = i * SLOT_UNROLL + u
            parent = ids_ref[0, s]
            at = pl.ds(pl.multiple_of(s * 8, 8), 8)
            for g in range(kv_heads):
                q = qs_ref[g, at, :].astype(bf16)
                score = dot_nt(q, cache_ref[parent, 0, g]) * scale
                top = jnp.max(score, axis=1, keepdims=True)
                e = jnp.exp(score - top)
                total = jnp.sum(e, axis=1, keepdims=True)
                o = dot(e.astype(bf16), cache_ref[parent, 1, g])
                os_ref[g, at, :] = o / total
                ls_ref[g, at, :] = jnp.broadcast_to(top + jnp.log(total), (8, head_dim))
        return carry

    lax.fori_loop(0, slots // SLOT_UNROLL, step, 0)
    lane = iota((slots, head_dim), 1)
    halves = []
    kv_width = kv_ref.shape[1] // kv_heads
    for g in range(kv_heads):
        pieces = []
        stat = jnp.zeros((slots, head_dim), f32)
        for h in range(group):
            pieces.append(os_ref[g, pl.ds(h, slots, stride=8), :].astype(bf16))
            stat = jnp.where(
                lax.bitwise_and(lane, 15) == h, ls_ref[g, pl.ds(h, slots, stride=8), :], stat
            )
        high = stat.astype(bf16).astype(f32)
        rest = stat - high
        middle = rest.astype(bf16).astype(f32)
        low = rest - middle
        pieces.append(kv_ref[:, g * kv_width : (g + 1) * kv_width])
        pieces.append(jnp.where(lane < 16, high, jnp.where(lane < 32, middle, low)).astype(bf16))
        halves.append(jnp.concatenate(pieces, axis=1))
    pack = pack_matrix(out_ref.shape[0], kv_heads, capacity, iota((1, slots), 1))
    out_ref[...] = dot(pack, jnp.concatenate(halves, axis=0)).astype(bf16)


def prefix_kernel(capacity, scale, block, idx_smem, idx_ref, qbox_ref, cache_ref, o_ref, lse_ref, qs_ref, acc_ref, m_ref, l_ref):
    children = idx_ref.shape[1]
    rows, width = qbox_ref.shape
    head_dim = cache_ref.shape[-1]
    kv_heads = cache_ref.shape[1]
    group = width // head_dim
    tiles = children // CHILD_TILE
    tile_rows = CHILD_TILE * group
    per_chunk = CHUNK // block
    base_col = to_column(idx_ref[0:1, :].astype(f32)).astype(i32)
    len_col = to_column(idx_ref[1:2, :].astype(f32)).astype(i32)
    for g in range(kv_heads):
        take = onehot(iota((children, rows), 1) == base_col + g * capacity)
        q = dot(take, qbox_ref[...]).astype(bf16)
        for t in range(tiles):
            for h in range(group):
                at = t * tile_rows + h * CHILD_TILE
                qs_ref[g, at : at + CHILD_TILE, :] = q[
                    t * CHILD_TILE : (t + 1) * CHILD_TILE, h * head_dim : (h + 1) * head_dim
                ]

    for t in range(tiles):
        at = slice(t * tile_rows, (t + 1) * tile_rows)
        lens = jnp.broadcast_to(len_col[t * CHILD_TILE : (t + 1) * CHILD_TILE], (CHILD_TILE, head_dim))
        lens = jnp.concatenate([lens] * group, axis=0)
        longest = idx_smem[1, t * CHILD_TILE]
        for g in range(kv_heads):
            acc_ref[g] = jnp.zeros((tile_rows, head_dim), f32)
            m_ref[g] = jnp.full((tile_rows, head_dim), LOW, f32)
            l_ref[g] = jnp.zeros((tile_rows, head_dim), f32)

        def step(j, carry):
            keys = pl.ds(pl.multiple_of(j * CHUNK, CHUNK), CHUNK)
            for g in range(kv_heads):
                score = dot_nt(qs_ref[g, at, :], cache_ref[0, g, keys, :])
                parts = []
                for b in range(per_chunk):
                    piece = score[:, b * block : (b + 1) * block] * scale
                    parts.append(jnp.where(lens > j * per_chunk + b, piece, LOW))
                top = functools.reduce(jnp.maximum, parts)
                old = m_ref[g]
                new = jnp.maximum(old, jnp.max(top, axis=1, keepdims=True))
                alpha = jnp.exp2(old - new)
                parts = [jnp.exp2(piece - new) for piece in parts]
                m_ref[g] = new
                l_ref[g] = l_ref[g] * alpha + functools.reduce(jnp.add, parts)
                e = jnp.concatenate([piece.astype(bf16) for piece in parts], axis=1)
                acc_ref[g] = acc_ref[g] * alpha + dot(e, cache_ref[1, g, keys, :])
            return carry

        lax.fori_loop(0, (longest + per_chunk - 1) // per_chunk, step, 0)
        for g in range(kv_heads):
            total = jnp.sum(l_ref[g], axis=1, keepdims=True)
            o_ref[g, at, :] = acc_ref[g] * (1.0 / total)
            lse_ref[g, at, :] = m_ref[g] * (1.0 / LOG2E) + jnp.log(total)


def merge_kernel(capacity, idx_ref, box_ref, o_ref, lse_ref, ctx_ref, kv_ref):
    children = idx_ref.shape[1]
    rows = box_ref.shape[0]
    kv_heads, _, head_dim = o_ref.shape
    group = o_ref.shape[1] // children
    tiles = children // CHILD_TILE
    tile_rows = CHILD_TILE * group
    kv_width = kv_ref.shape[1] // kv_heads
    base_col = to_column(idx_ref[0:1, :].astype(f32)).astype(i32)
    srank_col = to_column(idx_ref[2:3, :].astype(f32)).astype(i32)
    unsort = onehot(srank_col == iota((children, children), 1))
    contexts, values = [], []
    for g in range(kv_heads):
        take = onehot(iota((children, rows), 1) == base_col + g * capacity)
        got = dot(take, box_ref[...])
        stat = got[:, group * head_dim + kv_width :]
        for h in range(group):
            far_lse = stat[:, h : h + 1] + stat[:, 16 + h : 17 + h] + stat[:, 32 + h : 33 + h]
            share = got[:, h * head_dim : (h + 1) * head_dim]
            pick = [slice(t * tile_rows + h * CHILD_TILE, t * tile_rows + (h + 1) * CHILD_TILE) for t in range(tiles)]
            near = jnp.concatenate([o_ref[g, at, :] for at in pick], axis=0)
            near_lse = jnp.concatenate([lse_ref[g, at, :] for at in pick], axis=0)
            part = 1.0 / (1.0 + jnp.exp(far_lse - near_lse))
            rest = 1.0 / (1.0 + jnp.exp(near_lse - far_lse))
            contexts.append((near * part + share * rest).astype(bf16))
        values.append(got[:, group * head_dim : group * head_dim + kv_width].astype(bf16))
    ctx_ref[...] = dot(unsort, jnp.concatenate(contexts, axis=1)).astype(bf16)
    kv_ref[...] = dot(unsort, jnp.concatenate(values, axis=1)).astype(bf16)


def params(mib, **kw):
    return pltpu.CompilerParams(vmem_limit_bytes=mib * 2**20, **kw)


def shape(dims, dtype):
    return jax.ShapeDtypeStruct(dims, dtype)


def exchange(box, devices):
    rows, width = box.shape
    out = lax.all_to_all(
        box.reshape(devices, rows // devices, width), ("row", "col"), split_axis=0, concat_axis=0, tiled=True
    )
    return out.reshape(rows, width)


def local(child_parent, prefix_len, child_delta, parent_hidden, parent_cache, prefix_cache, norm_gain, w_query, w_kv):
    row_count, col_count = lax.axis_size("row"), lax.axis_size("col")
    devices = row_count * col_count
    children, features = child_delta.shape
    parents = parent_hidden.shape[0]
    capacity = 2 * ((children // (2 * col_count) + row_count - 1) // row_count)
    slots = devices * capacity
    parts = max(1, 8 // capacity)
    kv_heads, block, head_dim = parent_cache.shape[2], parent_cache.shape[3], parent_cache.shape[4]
    query_width = w_query.shape[1]
    half = query_width // kv_heads
    group = half // head_dim
    scale = 1.0 / math.sqrt(head_dim)
    box_count = slots * kv_heads

    box, idx, ids = pl.pallas_call(
        functools.partial(pack_kernel, parents, capacity, parts, slots),
        out_shape=(
            shape((slots * parts, features // parts), bf16),
            shape((8, children), i32),
            shape((1, slots), i32),
        ),
        in_specs=[VMEM] * 3,
        out_specs=(VMEM, VMEM, VMEM),
        compiler_params=params(12),
        name="pack",
    )(child_parent.reshape(1, children), prefix_len.reshape(1, children), child_delta)
    far_box = exchange(box, devices)
    far_ids = lax.all_to_all(
        ids.reshape(devices, capacity), ("row", "col"), split_axis=0, concat_axis=0, tiled=True
    ).reshape(1, slots)

    queries, query_box, new_kv = pl.pallas_call(
        functools.partial(project_kernel, capacity, parts),
        out_shape=(
            shape((slots, query_width), bf16),
            shape((box_count, half), bf16),
            shape((slots, w_kv.shape[1]), bf16),
        ),
        in_specs=[VMEM] * 6,
        out_specs=(VMEM, VMEM, VMEM),
        scratch_shapes=[pltpu.VMEM((slots, features), f32), pltpu.VMEM((slots, features), bf16)],
        compiler_params=params(32),
        name="project",
    )(far_box, far_ids, parent_hidden, norm_gain.reshape(1, features), w_query, w_kv)
    near_query = exchange(query_box, devices)

    share_width = half + w_kv.shape[1] // kv_heads + head_dim
    share_box = pl.pallas_call(
        functools.partial(parent_kernel, capacity, scale),
        out_shape=shape((box_count, share_width), bf16),
        in_specs=[SMEM, VMEM, VMEM, VMEM],
        out_specs=VMEM,
        scratch_shapes=[pltpu.VMEM((kv_heads, slots * 8, head_dim), f32)] * 3,
        compiler_params=params(16),
        name="parent_attend",
    )(far_ids, queries, new_kv, parent_cache)
    near_share = exchange(share_box, devices)

    tile_rows = CHILD_TILE * group
    near, near_lse = pl.pallas_call(
        functools.partial(prefix_kernel, capacity, scale * LOG2E, block),
        out_shape=(
            shape((kv_heads, children * group, head_dim), f32),
            shape((kv_heads, children * group, head_dim), f32),
        ),
        in_specs=[SMEM, VMEM, VMEM, VMEM],
        out_specs=(VMEM, VMEM),
        scratch_shapes=[pltpu.VMEM((kv_heads, children * group, head_dim), bf16)]
        + [pltpu.VMEM((kv_heads, tile_rows, head_dim), f32)] * 3,
        compiler_params=params(20),
        name="prefix_attend",
    )(idx, idx, near_query, prefix_cache[0])

    return pl.pallas_call(
        functools.partial(merge_kernel, capacity),
        out_shape=(shape((children, query_width), bf16), shape((children, w_kv.shape[1]), bf16)),
        in_specs=[VMEM] * 4,
        out_specs=(VMEM, VMEM),
        compiler_params=params(16),
        name="merge",
    )(idx, near_share, near, near_lse)


def solution(mesh):
    spec = ("row", "col")
    return jax.shard_map(
        local,
        mesh=mesh,
        in_specs=(
            P(spec),
            P(spec),
            P(spec, None),
            P(spec, None),
            P(spec, None, None, None, None),
            P(spec, None, None, None, None),
            P(),
            P(),
            P(),
        ),
        out_specs=(P(spec, None), P(spec, None)),
        check_vma=False,
    )
```
